32 devices in a mesh: parts: 2 (over x), virt: 16 (over z, y, core).
Axes of the slice: x: 2, y: 2, z: 4, core: 2. Of those that a mesh axis runs over, the one named last changes fastest.
Arguments:
- trials: float32 [4096, 4, 256], P(('parts', 'virt')), parts along dimension 0, may hold values from -6 to 6
- vv_vectors: float32 [48, 2048, 2048], P('parts', 'virt'), parts along dimension 0, may hold values from -0.125 to 0.125
- oo_vectors: float32 [48, 256, 256], P('parts'), parts along dimension 0, may hold values from -0.078125 to 0.078125
- occ_energy: float32 [512], P('parts'), parts along dimension 0, may hold values from -2 to -0.5
- virt_energy: float32 [4096], P(('parts', 'virt')), parts along dimension 0, may hold values from 0.5 to 5, as said below
Outputs:
- filtered: float32 [4096, 4, 256], P(('parts', 'virt')), parts along dimension 0
- gram: float32 [8, 4], P('parts'), parts along dimension 0
The draws below stay inside these ranges and needn't reach their ends.
There are 2 independent parts, one for each index of `parts`. The reference program is written for one: setup_inputs(seed, part) draws one part's arguments, and reference() takes and returns one part's arrays. A program takes and returns all parts, laid end to end along the dimension named above; each array names one. Nothing has to cross between parts.
Inputs may be any that keep to these rules, and one draw needn't show every extreme that they name: `virt_energy`: rises with the orbital index, with a rough jitter.
All inputs are finite; a program needn't handle non-finite values.
Results may differ from the reference program's by a relative error of at most 0.0001.
Values sent between devices are 32-bit elements; how exact they have to be, the bound alone decides.
No kernel may reach another device: no remote copies, remote signals or barrier semaphores. Data moves between devices by JAX's collectives and lax.ppermute only.
A program may use at most 128 MiB of HBM per device.

```python
import jax
import jax.numpy as jnp
from jax import lax

O = 256
V = 2048
K = 4
NVEC = 24


def draw_virt_energy(key, part):
    ladder = 0.5 + 3.5 * jnp.arange(V, dtype=jnp.float32) / V
    jitter = jax.random.uniform(key, (V,), jnp.float32, 0.0, 0.5)
    return ladder + jitter


def shard_levels(rng, dims, cuts, smallest, top_value):
    def one(position, shards_of):
        steps = jax.random.uniform(jax.random.fold_in(jax.random.fold_in(rng, 6), position), (shards_of,), jnp.float32, smallest / len(cuts), top_value / len(cuts))
        return jnp.repeat(jnp.exp(steps), dims[position] // shards_of).reshape((-1,) + (1,) * (len(dims) - position - 1))

    level = one(*cuts[0])
    for cut in cuts[1:]:
        level = level * one(*cut)
    return level


def centred(own_key, shape, scale, most, cuts=(), held_as=jnp.bfloat16):
    entries = scale * jax.random.normal(own_key, shape, jnp.float32)
    if cuts:
        entries = entries * shard_levels(own_key, shape, cuts, -0.22, 0.18)
    return jnp.clip(entries, -most, most).astype(held_as)


def setup_inputs(seed: int = 0, part: int = 0) -> dict:
    splits = jax.random.split(jax.random.key(seed), 6)
    part_splits = jax.random.split(jax.random.fold_in(splits[5], part), 6)
    return {
        "trials": centred(part_splits[0], (V, K, O), 1.0, 6.0, ((0, 16),), jnp.float32),
        "vv_vectors": centred(part_splits[1], (NVEC, V, V), V ** -0.5, 0.125, ((1, 16),), jnp.float32),
        "oo_vectors": centred(part_splits[2], (NVEC, O, O), (O * NVEC) ** -0.5, 0.078125, (), jnp.float32),
        "occ_energy": jnp.clip(jax.random.uniform(part_splits[3], (O,), jnp.float32, -2.0, -0.5), -2.0, -0.5),
        "virt_energy": draw_virt_energy(jax.random.fold_in(jax.random.fold_in(splits[5], part), 71), part),
    }


HIGH = lax.Precision.HIGHEST


def apply_operator(trial_block, vv_vectors, oo_vectors, energy_gap):
    flattened = trial_block.reshape(V, K * O)

    def per_vector(running, vectors):
        vv_one, oo_one = vectors
        half_image = jnp.dot(vv_one, flattened, precision=HIGH).reshape(V, K, O)
        return running + jnp.einsum("akj,ji->aki", half_image, oo_one, precision=HIGH), None

    direct, _ = lax.scan(per_vector, jnp.zeros((V, K, O), jnp.float32), (vv_vectors, oo_vectors))
    return energy_gap * trial_block - direct


def reference(trials, vv_vectors, oo_vectors, occ_energy, virt_energy):
    energy_gap = (virt_energy[:, None] - occ_energy[None, :])[:, None, :]
    first = (apply_operator(trials, vv_vectors, oo_vectors, energy_gap) - 4.5 * trials) / 3.0
    filtered = 2.0 * (apply_operator(first, vv_vectors, oo_vectors, energy_gap) - 4.5 * first) / 3.0 - trials
    gram = jnp.einsum("aki,ali->kl", filtered, filtered, precision=HIGH) / (O * V)
    return filtered, gram
```

```python
import functools

import jax
import jax.numpy as jnp
from jax import lax
from jax.experimental import pallas as pl
from jax.experimental.pallas import tpu as pltpu
from jax.sharding import PartitionSpec as P


HIGH = lax.Precision.HIGHEST
LANES = 128
STEP = 4


def split(x):
    high = x.astype(jnp.bfloat16)
    return high, (x - high.astype(jnp.float32)).astype(jnp.bfloat16)


def dot3(a, b):
    (a_high, a_low), (b_high, b_low) = a, b
    dot = functools.partial(jnp.dot, preferred_element_type=jnp.float32)
    return dot(a_high, b_high) + (dot(a_high, b_low) + dot(a_low, b_high))


def direct_kernel(index_ref, *refs, fields, blocks, width):
    field_refs, vv_refs, oo_ref, out_ref, high_ref, low_ref, acc_ref = (
        refs[:fields],
        refs[fields : fields + blocks],
        *refs[fields + blocks :],
    )
    step = pl.program_id(0)
    rows = vv_refs[0].shape[1]
    trials = out_ref.shape[1] // width

    @pl.when(step == 0)
    def _():
        at = 0
        for ref in field_refs:
            high, low = split(ref[...])
            high_ref[at : at + ref.shape[0], :] = high
            low_ref[at : at + ref.shape[0], :] = low
            at += ref.shape[0]
        acc_ref[...] = jnp.zeros_like(acc_ref)

    vv = jnp.concatenate([ref[...].reshape(-1, LANES) for ref in vv_refs], axis=1)
    half = dot3(split(vv), (high_ref[...], low_ref[...]))
    vectors = range(vv_refs[0].shape[0])
    turned = jnp.concatenate(
        [
            jnp.concatenate(
                [half[p * rows : (p + 1) * rows, k * width : (k + 1) * width] for p in vectors], axis=1
            )
            for k in range(trials)
        ],
        axis=0,
    )
    oo = split(oo_ref[...].reshape(-1, width))
    high, low = split(turned)
    middle = high.shape[0] // 2
    for at in (slice(0, middle), slice(middle, 2 * middle)):
        acc_ref[at, :] += dot3((high[at], low[at]), oo)

    @pl.when(step == pl.num_programs(0) - 1)
    def _():
        for k in range(trials):
            out_ref[:, k * width : (k + 1) * width] = acc_ref[k * rows : (k + 1) * rows, :]


def direct_part(fields, indices, vv_vectors, oo_vectors):
    count, rows, _ = vv_vectors.shape
    width = oo_vectors.shape[-1]
    columns = fields[0].shape[1]
    blocks = len(indices)
    step = STEP if count % STEP == 0 else 1
    whole = lambda shape: pl.BlockSpec(shape, lambda i, s: (0,) * len(shape))
    flops = 6 * count * rows * columns * (blocks * LANES + width)
    return pl.pallas_call(
        functools.partial(direct_kernel, fields=len(fields), blocks=blocks, width=width),
        grid_spec=pltpu.PrefetchScalarGridSpec(
            num_scalar_prefetch=1,
            grid=(count // step,),
            in_specs=[whole(f.shape) for f in fields]
            + [pl.BlockSpec((step, rows, LANES), lambda i, s, b=b: (i, 0, s[b])) for b in range(blocks)]
            + [pl.BlockSpec((step, width, width), lambda i, s: (i, 0, 0))],
            out_specs=whole((rows, columns)),
            scratch_shapes=[
                pltpu.VMEM((blocks * LANES, columns), jnp.bfloat16),
                pltpu.VMEM((blocks * LANES, columns), jnp.bfloat16),
                pltpu.VMEM((rows * columns // width, width), jnp.float32),
            ],
        ),
        out_shape=jax.ShapeDtypeStruct((rows, columns), jnp.float32),
        cost_estimate=pl.CostEstimate(flops=flops, bytes_accessed=4 * count * rows * blocks * LANES, transcendentals=0),
        compiler_params=pltpu.CompilerParams(dimension_semantics=("arbitrary",), vmem_limit_bytes=56 * 2**20),
    )(jnp.stack(indices).astype(jnp.int32), *fields, *([vv_vectors] * blocks), oo_vectors)


def exchange(x, mask):
    n = lax.axis_size("virt")
    return lax.ppermute(x, "virt", [(v, v ^ mask) for v in range(n)])


def apply_direct(x, vv_vectors, oo_vectors):
    me = lax.axis_index("virt")
    core, side = 1, 2
    lines = list(range(4, lax.axis_size("virt"), 4))
    part = functools.partial(direct_part, vv_vectors=vv_vectors, oo_vectors=oo_vectors)

    def pair(masks):
        return [me ^ m for m in masks] + [me ^ m ^ core for m in masks]

    own = exchange(x, core)
    near = lines[:1]
    far = lines[1:]
    across = exchange(x, side)
    along = [exchange(x, m) for m in near]
    along += [exchange(x, m) for m in far]
    total = part([x, own], [me, me ^ core])
    mine = [across] + along[:1]
    mine += [exchange(jnp.concatenate(mine), core)]
    crossed = [exchange(a, side) for a in along[:1]]
    crossed += [exchange(a, side) for a in along[1:]]
    total = total + part(mine, pair([side] + near))
    if far:
        mid = far + [m ^ side for m in near]
        mine = along[1:] + crossed[:1]
        mine += [exchange(jnp.concatenate(mine), core)]
        total = total + part(mine, pair(mid))
    last = [m ^ side for m in (far if far else near)]
    mine = crossed[1:] if far else crossed
    return total + part(mine + [exchange(jnp.concatenate(mine), core)], pair(last))


def per_device_exchange(trials, vv_vectors, oo_vectors, occ_energy, virt_energy):
    rows, count, width = trials.shape
    n = lax.axis_size("virt")
    start = trials.reshape(rows, count * width)
    gap = virt_energy[:, None] - jnp.tile(occ_energy, count)[None, :]
    first = (gap * start - apply_direct(start, vv_vectors, oo_vectors) - 4.5 * start) / 3.0
    image = gap * first - apply_direct(first, vv_vectors, oo_vectors)
    filtered = (2.0 * (image - 4.5 * first) / 3.0 - start).reshape(rows, count, width)
    gram = jnp.einsum("aki,ali->kl", filtered, filtered, precision=HIGH)
    mask = 1
    while mask < n:
        gram = gram + exchange(gram, mask)
        mask *= 2
    return filtered, gram / (width * rows * n)


def apply_gathered(trial_block, vv_vectors, oo_vectors, energy_gap):
    local_rows, count, width = trial_block.shape
    gathered = lax.all_gather(trial_block, "virt", axis=0, tiled=True)
    flattened = gathered.reshape(gathered.shape[0], count * width)
    half_image = jnp.einsum("pab,bm->pam", vv_vectors, flattened, precision=HIGH)
    half_image = half_image.reshape(vv_vectors.shape[0], local_rows, count, width)
    direct = jnp.einsum("pakj,pji->aki", half_image, oo_vectors, precision=HIGH)
    return energy_gap * trial_block - direct


def per_device_gathered(trials, vv_vectors, oo_vectors, occ_energy, virt_energy):
    energy_gap = (virt_energy[:, None] - occ_energy[None, :])[:, None, :]
    apply_operator = functools.partial(
        apply_gathered, vv_vectors=vv_vectors, oo_vectors=oo_vectors, energy_gap=energy_gap
    )
    first = (apply_operator(trials) - 4.5 * trials) / 3.0
    filtered = 2.0 * (apply_operator(first) - 4.5 * first) / 3.0 - trials
    partial_gram = jnp.einsum("aki,ali->kl", filtered, filtered, precision=HIGH)
    gram = lax.psum(partial_gram, "virt") / (
        occ_energy.shape[0] * trials.shape[0] * lax.axis_size("virt")
    )
    return filtered, gram


def per_device(trials, *rest):
    n = lax.axis_size("virt")
    whole_blocks = trials.shape[0] == LANES and trials.shape[2] % LANES == 0
    few = n & (n - 1) == 0 and 8 <= n <= 16
    return (per_device_exchange if whole_blocks and few else per_device_gathered)(trials, *rest)


def solution(mesh):
    in_specs = (
        P(("parts", "virt"), None, None),
        P("parts", "virt", None),
        P("parts", None, None),
        P("parts"),
        P(("parts", "virt")),
    )
    out_specs = (P(("parts", "virt"), None, None), P("parts", None))
    return jax.shard_map(
        per_device, mesh=mesh, in_specs=in_specs, out_specs=out_specs, check_vma=False
    )
```
